32 devices in a mesh: row: 8 (over z, y), expert: 4 (over x, core).
Axes of the slice: x: 2, y: 2, z: 4, core: 2. Of those that a mesh axis runs over, the one named last changes fastest.
Arguments:
- base: bfloat16 [8, 7168, 2048], P('expert', 'row'), may hold values from -6 to 6
- left_factors: bfloat16 [8, 7168, 64], P('expert', None, 'row'), may hold values from -6 to 6
- right_factors: bfloat16 [8, 64, 2048], P('expert', None, 'row'), may hold values from -0.75 to 0.75
- expert_adapter_scale: float32 [8], P('expert'), may hold values from 0.5 to 2
- placement: int32 [8], P('expert'), may hold values from 0 to 3, as said below
Outputs:
- serving: bfloat16 [8, 7168, 2048], P('expert', None, 'row')
The draws below stay inside these ranges and needn't reach their ends.
Inputs may be any that keep to these rules, and one draw needn't show every extreme that they name: `placement`: expert g * 2 + j is placed on (g + o_j) mod (4) for one offset o_j per slot j, the same for every g; the offsets of slots 0 and 1 add up to 3.
All inputs are finite; a program needn't handle non-finite values.
Results may differ from the reference program's by a relative error of at most 0.001.
Values may be sent and summed in bfloat16 or wider, within the bound.
A program may use at most 64 MiB of HBM per device.

```python
import math
import jax
import jax.numpy as jnp
from jax import lax

MODEL_WIDTH = 7168
HIDDEN_UNITS = 2048
ADAPTER_RANK = 64
EXP_DEV = 2
EXPERT_TOTAL = 8


def draw_placement(key, part):
    group_count = EXPERT_TOTAL // EXP_DEV
    offsets = jax.random.randint(jax.random.fold_in(key, 17), (EXP_DEV,), 0, group_count)
    offsets = offsets.at[1].set(group_count - 1 - offsets[0])
    expert_ids = jnp.arange(EXPERT_TOTAL, dtype=jnp.int32)
    group_ids = expert_ids // EXP_DEV
    slot_ids = expert_ids % EXP_DEV
    return jnp.mod(group_ids + offsets[slot_ids], group_count).astype(jnp.int32)


def shard_levels(rng, shape, shards, smallest, top_value):
    def one(position, parts):
        draws = jax.random.uniform(jax.random.fold_in(jax.random.fold_in(rng, 6), position), (parts,), jnp.float32, smallest / len(shards), top_value / len(shards))
        return jnp.repeat(jnp.exp(draws), shape[position] // parts).reshape((-1,) + (1,) * (len(shape) - position - 1))

    factor_of = one(*shards[0])
    for cut in shards[1:]:
        factor_of = factor_of * one(*cut)
    return factor_of


def gaussian(stream_key, dims, spread, reach, split=(), kind=jnp.bfloat16):
    drawn = spread * jax.random.normal(stream_key, dims, jnp.float32)
    if split:
        drawn = drawn * shard_levels(stream_key, dims, split, -0.22, 0.18)
    return jnp.clip(drawn, -reach, reach).astype(kind)


def setup_inputs(seed: int = 0) -> dict:
    seeds = jax.random.split(jax.random.key(seed), 6)
    return {
        "base": gaussian(seeds[0], (EXPERT_TOTAL, MODEL_WIDTH, HIDDEN_UNITS), 1.0, 6.0, ((0, 4), (1, 8))),
        "left_factors": gaussian(seeds[1], (EXPERT_TOTAL, MODEL_WIDTH, ADAPTER_RANK), 1.0, 6.0, ((0, 4), (2, 8))),
        "right_factors": gaussian(seeds[2], (EXPERT_TOTAL, ADAPTER_RANK, HIDDEN_UNITS), ADAPTER_RANK ** -0.5, 0.75, ((0, 4), (2, 8))),
        "expert_adapter_scale": jnp.clip(jnp.exp(math.log(2.0) - 1.3862944 * jax.random.uniform(seeds[3], (EXPERT_TOTAL,), jnp.float32) ** shard_levels(seeds[3], (EXPERT_TOTAL,), ((0, 4),), -0.2, 0.2)), 0.5, 2.0),
        "placement": draw_placement(jax.random.fold_in(seeds[5], 71), 0),
    }


def combine_expert_weight(expert_items):
    tile_base, factor_b, factor_a, scale_one = expert_items
    weight_update = jnp.dot(factor_b, factor_a, preferred_element_type=jnp.float32)
    return (tile_base.astype(jnp.float32) + scale_one * weight_update).astype(jnp.bfloat16)


def reference(base, left_factors, right_factors, expert_adapter_scale, placement):
    combined_weight = lax.map(combine_expert_weight, (base, left_factors, right_factors, expert_adapter_scale))
    slot_index = jnp.arange(EXPERT_TOTAL, dtype=jnp.int32) % EXP_DEV
    target = placement.astype(jnp.int32) * EXP_DEV + slot_index
    return jnp.zeros_like(combined_weight).at[target].set(combined_weight)
```

```python
import functools

import jax
import jax.numpy as jnp
from jax import lax
from jax.experimental import pallas as pl
from jax.experimental.pallas import tpu as pltpu
from jax.sharding import PartitionSpec as P

MESH = pl.DeviceIdType.MESH
WINDOW = 8


def piece_order(rows):
    half = rows // 2
    order = []
    for m in range(half):
        order += [half + m, m] if m else [half]
    return order + [0]


def exchange_kernel(dist, groups, rows, base, left, right, scale, got, left_all, right_got, scale_got,
                    bounce, send, recv, lsend, lrecv, ssend, srecv, own):
    r, g = lax.axis_index("row"), lax.axis_index("expert")
    slots, height = base.shape[0], base.shape[1]
    width = base.shape[2] // rows
    to = [lax.rem(g + d, groups) for d in dist]

    barrier = pltpu.get_barrier_semaphore()
    steps = sorted({d for d in dist} | {(groups - d) % groups for d in dist} | {0})
    for e in steps:
        for m in range(rows):
            if e == 0 and m == 0:
                continue
            pl.semaphore_signal(barrier, inc=1, device_id={"row": r ^ m, "expert": lax.rem(g + e, groups)},
                                device_id_type=MESH)
    pl.semaphore_wait(barrier, len(steps) * rows - 1)

    def remote(src, dst, s, t, row, expert):
        return pltpu.make_async_remote_copy(src_ref=src, dst_ref=dst, send_sem=s, recv_sem=t,
                                            device_id={"row": row, "expert": expert}, device_id_type=MESH)

    first = []
    for j in range(slots):
        for src, dst, s, t in (
            (left.at[j], left_all.at[j, r], lsend.at[j, 0], lrecv.at[j, 0]),
            (right.at[j], right_got.at[j], ssend.at[j, 0], srecv.at[j, 0]),
            (scale.at[j], scale_got.at[j], ssend.at[j, 1], srecv.at[j, 1]),
        ):
            if dist[j] == 0:
                copy = pltpu.make_async_copy(src, dst, t)
            else:
                copy = remote(src, dst, s, t, r, to[j])
            copy.start()
            first.append(copy)

    def left_round(mask, held):
        copies = []
        for s in held:
            for j in range(slots):
                piece = left_all.at[j, r ^ s]
                copy = remote(piece, piece, lsend.at[j, mask | s], lrecv.at[j, mask | s], r ^ mask, g)
                copy.start()
                copies.append(copy)
        return copies

    rounds = []
    mask, held = rows // 2, [0]
    while mask:
        rounds.append((mask, list(held)))
        held += [s | mask for s in held]
        mask //= 2

    pieces = [(m, j) for m in piece_order(rows) for j in range(slots)]
    at = {(i + 1) * len(pieces) // (len(rounds) + 2): i for i in range(len(rounds))}
    pending, sent, waiting = [], [], first
    for k, (m, j) in enumerate(pieces):
        if k in at:
            for copy in waiting:
                copy.wait()
            waiting = left_round(*rounds[at[k]])
        if len(pending) >= WINDOW:
            pending.pop(0).wait_send()
        c = r ^ m
        src = base.at[j, :, pl.ds(pl.multiple_of(c * width, width), width)]
        if m == 0 and dist[j] == 0:
            copy = pltpu.make_async_copy(src, bounce, own)
            copy.start()
            copy.wait()
            copy = pltpu.make_async_copy(bounce, got.at[j, r], own)
            copy.start()
            last = copy
            sent.append(copy.wait)
        else:
            copy = remote(src, got.at[j, r], send.at[j, m], recv.at[j, m], c, to[j])
            copy.start()
            pending.append(copy)
            sent.append(copy.wait_recv)
    for copy in waiting:
        copy.wait()
    for copy in pending:
        copy.wait_send()
    for wait in sent:
        wait()


def exchange(first, groups, rows, base, left, right, scale):
    dist = (first, groups - 1 - first)
    slots, height, total = base.shape
    width = total // rows
    rank, model = left.shape[1:]
    anywhere = pl.BlockSpec(memory_space=pl.ANY)
    dma = pltpu.SemaphoreType.DMA
    return pl.pallas_call(
        functools.partial(exchange_kernel, dist, groups, rows),
        out_shape=(
            jax.ShapeDtypeStruct((slots, rows, height, width), base.dtype),
            jax.ShapeDtypeStruct((slots, rows, rank, model), left.dtype),
            jax.ShapeDtypeStruct(right.shape, right.dtype),
            jax.ShapeDtypeStruct(scale.shape, scale.dtype),
        ),
        in_specs=[anywhere] * 4,
        out_specs=[anywhere] * 4,
        scratch_shapes=[
            pltpu.VMEM((height, width), base.dtype),
            dma((slots, rows)), dma((slots, rows)),
            dma((slots, rows)), dma((slots, rows)),
            dma((slots, 2)), dma((slots, 2)),
            dma,
        ],
        compiler_params=pltpu.CompilerParams(collective_id=first, has_side_effects=True),
        name=f"exchange_{first}",
    )(base, left, right, scale)


def merge_kernel(base, left, right, scale, out):
    delta = lax.dot_general(left[0], right[0], (((0,), (0,)), ((), ())), preferred_element_type=jnp.float32)
    out[0] = (base[0].astype(jnp.float32) + scale[0, 0:1, 0:1] * delta).astype(out.dtype)


def merge(base, left, right, scale):
    slots, model, width = base.shape
    rank = left.shape[1]
    block = next(b for b in (1024, 512, 256, 128) if model % b == 0)
    return pl.pallas_call(
        merge_kernel,
        grid=(slots, model // block),
        in_specs=[
            pl.BlockSpec((1, block, width), lambda j, i: (j, i, 0)),
            pl.BlockSpec((1, rank, block), lambda j, i: (j, 0, i)),
            pl.BlockSpec((1, rank, width), lambda j, i: (j, 0, 0)),
            pl.BlockSpec((1,) + scale.shape[1:], lambda j, i: (j, 0, 0)),
        ],
        out_specs=pl.BlockSpec((1, block, width), lambda j, i: (j, i, 0)),
        out_shape=jax.ShapeDtypeStruct(base.shape, base.dtype),
        compiler_params=pltpu.CompilerParams(dimension_semantics=("arbitrary", "arbitrary")),
        name="merge",
    )(base, left, right, scale)


def local(groups, rows, base, left_factors, right_factors, expert_adapter_scale, placement):
    first = jnp.mod(placement[0] - lax.axis_index("expert"), groups)
    slots = base.shape[0]
    left = jnp.swapaxes(left_factors, 1, 2)
    scale = jnp.broadcast_to(expert_adapter_scale[:, None, None], (slots, 8, 128))
    got, left_all, right, scale = lax.switch(
        first,
        [functools.partial(exchange, o, groups, rows) for o in range(groups)],
        base, left, right_factors, scale,
    )
    model = left.shape[2]
    return merge(
        got.reshape(slots, model, got.shape[3]),
        left_all.reshape(slots, -1, model),
        right,
        scale,
    )


def solution(mesh):
    placed = (
        P("expert", "row", None),
        P("expert", None, "row"),
        P("expert", None, "row"),
        P("expert"),
        P("expert"),
    )
    return jax.shard_map(
        functools.partial(local, mesh.shape["expert"], mesh.shape["row"]),
        mesh=mesh, in_specs=placed, out_specs=P("expert", None, "row"), check_vma=False,
    )
```

```python
import functools

import jax
import jax.numpy as jnp
from jax import lax
from jax.experimental import pallas as pl
from jax.experimental.pallas import tpu as pltpu
from jax.sharding import PartitionSpec as P

MESH = pl.DeviceIdType.MESH
WINDOW = 8


def piece_order(rows):
    half = rows // 2
    near = sorted(range(half), key=lambda m: (m == 0, m != half // 2, m))
    return [m for pair in zip(range(half, rows), near) for m in pair]


def exchange_kernel(dist, groups, rows, base, left, right, scale, got, left_all, right_got, scale_got,
                    bounce, send, recv, lsend, lrecv, ssend, srecv, own):
    r, g = lax.axis_index("row"), lax.axis_index("expert")
    slots, height = base.shape[0], base.shape[1]
    width = base.shape[2] // rows
    to = [lax.rem(g + d, groups) for d in dist]

    barrier = pltpu.get_barrier_semaphore()
    steps = sorted({d for d in dist} | {(groups - d) % groups for d in dist} | {0})
    for e in steps:
        for m in range(rows):
            if e == 0 and m == 0:
                continue
            pl.semaphore_signal(barrier, inc=1, device_id={"row": r ^ m, "expert": lax.rem(g + e, groups)},
                                device_id_type=MESH)
    pl.semaphore_wait(barrier, len(steps) * rows - 1)

    def remote(src, dst, s, t, row, expert):
        return pltpu.make_async_remote_copy(src_ref=src, dst_ref=dst, send_sem=s, recv_sem=t,
                                            device_id={"row": row, "expert": expert}, device_id_type=MESH)

    first = []
    for j in range(slots):
        for src, dst, s, t in (
            (left.at[j], left_all.at[j, r], lsend.at[j, 0], lrecv.at[j, 0]),
            (right.at[j], right_got.at[j], ssend.at[j, 0], srecv.at[j, 0]),
            (scale.at[j], scale_got.at[j], ssend.at[j, 1], srecv.at[j, 1]),
        ):
            if dist[j] == 0:
                copy = pltpu.make_async_copy(src, dst, t)
            else:
                copy = remote(src, dst, s, t, r, to[j])
            copy.start()
            first.append(copy)

    def left_round(mask, held):
        copies = []
        for s in held:
            for j in range(slots):
                piece = left_all.at[j, r ^ s]
                copy = remote(piece, piece, lsend.at[j, mask | s], lrecv.at[j, mask | s], r ^ mask, g)
                copy.start()
                copies.append(copy)
        return copies

    rounds = []
    mask, held = rows // 2, [0]
    while mask:
        rounds.append((mask, list(held)))
        held += [s | mask for s in held]
        mask //= 2

    pieces = [(m, j) for m in piece_order(rows) for j in range(slots)]
    at = {1 + i * (len(pieces) // len(rounds)): i for i in range(len(rounds))}
    pending, sent, waiting = [], [], first
    for k, (m, j) in enumerate(pieces):
        if k in at:
            for copy in waiting:
                copy.wait()
            waiting = left_round(*rounds[at[k]])
        if len(pending) >= WINDOW:
            pending.pop(0).wait_send()
        c = r ^ m
        src = base.at[j, :, pl.ds(pl.multiple_of(c * width, width), width)]
        if m == 0 and dist[j] == 0:
            copy = pltpu.make_async_copy(src, bounce, own)
            copy.start()
            copy.wait()
            copy = pltpu.make_async_copy(bounce, got.at[j, r], own)
            copy.start()
            last = copy
            sent.append(copy.wait)
        else:
            copy = remote(src, got.at[j, r], send.at[j, m], recv.at[j, m], c, to[j])
            copy.start()
            pending.append(copy)
            sent.append(copy.wait_recv)
    for copy in waiting:
        copy.wait()
    for copy in pending:
        copy.wait_send()
    for wait in sent:
        wait()


def exchange(first, groups, rows, base, left, right, scale):
    dist = (first, groups - 1 - first)
    slots, height, total = base.shape
    width = total // rows
    rank, model = left.shape[1:]
    anywhere = pl.BlockSpec(memory_space=pl.ANY)
    dma = pltpu.SemaphoreType.DMA
    return pl.pallas_call(
        functools.partial(exchange_kernel, dist, groups, rows),
        out_shape=(
            jax.ShapeDtypeStruct((slots, rows, height, width), base.dtype),
            jax.ShapeDtypeStruct((slots, rows, rank, model), left.dtype),
            jax.ShapeDtypeStruct(right.shape, right.dtype),
            jax.ShapeDtypeStruct(scale.shape, scale.dtype),
        ),
        in_specs=[anywhere] * 4,
        out_specs=[anywhere] * 4,
        scratch_shapes=[
            pltpu.VMEM((height, width), base.dtype),
            dma((slots, rows)), dma((slots, rows)),
            dma((slots, rows)), dma((slots, rows)),
            dma((slots, 2)), dma((slots, 2)),
            dma,
        ],
        compiler_params=pltpu.CompilerParams(collective_id=first, has_side_effects=True),
        name=f"exchange_{first}",
    )(base, left, right, scale)


def merge_kernel(base, left, right, scale, out):
    delta = lax.dot_general(left[0], right[0], (((0,), (0,)), ((), ())), preferred_element_type=jnp.float32)
    out[0] = (base[0].astype(jnp.float32) + scale[0, 0:1, 0:1] * delta).astype(out.dtype)


def merge(base, left, right, scale):
    slots, model, width = base.shape
    rank = left.shape[1]
    block = next(b for b in (1024, 512, 256, 128) if model % b == 0)
    return pl.pallas_call(
        merge_kernel,
        grid=(slots, model // block),
        in_specs=[
            pl.BlockSpec((1, block, width), lambda j, i: (j, i, 0)),
            pl.BlockSpec((1, rank, block), lambda j, i: (j, 0, i)),
            pl.BlockSpec((1, rank, width), lambda j, i: (j, 0, 0)),
            pl.BlockSpec((1,) + scale.shape[1:], lambda j, i: (j, 0, 0)),
        ],
        out_specs=pl.BlockSpec((1, block, width), lambda j, i: (j, i, 0)),
        out_shape=jax.ShapeDtypeStruct(base.shape, base.dtype),
        compiler_params=pltpu.CompilerParams(dimension_semantics=("arbitrary", "arbitrary")),
        name="merge",
    )(base, left, right, scale)


def local(groups, rows, base, left_factors, right_factors, expert_adapter_scale, placement):
    first = jnp.mod(placement[0] - lax.axis_index("expert"), groups)
    slots = base.shape[0]
    left = jnp.swapaxes(left_factors, 1, 2)
    scale = jnp.broadcast_to(expert_adapter_scale[:, None, None], (slots, 8, 128))
    got, left_all, right, scale = lax.switch(
        first,
        [functools.partial(exchange, o, groups, rows) for o in range(groups)],
        base, left, right_factors, scale,
    )
    model = left.shape[2]
    return merge(
        got.reshape(slots, model, got.shape[3]),
        left_all.reshape(slots, -1, model),
        right,
        scale,
    )


def solution(mesh):
    placed = (
        P("expert", "row", None),
        P("expert", None, "row"),
        P("expert", None, "row"),
        P("expert"),
        P("expert"),
    )
    return jax.shard_map(
        functools.partial(local, mesh.shape["expert"], mesh.shape["row"]),
        mesh=mesh, in_specs=placed, out_specs=P("expert", None, "row"), check_vma=False,
    )
```

```python
import functools

import jax
import jax.numpy as jnp
from jax import lax
from jax.experimental import pallas as pl
from jax.experimental.pallas import tpu as pltpu
from jax.sharding import PartitionSpec as P

MESH = pl.DeviceIdType.MESH
WINDOW = 8
LANES = 128


def piece_order(rows):
    half = rows // 2
    return [m for q in range(half) for m in (half + q, (half // 2 + q) % half)]


def exchange_kernel(dist, groups, rows, base, left, right, scale, out, got, left_all, right_got, scale_got,
                    send, recv, lsend, lrecv, ssend, srecv, osem):
    r, g = lax.axis_index("row"), lax.axis_index("expert")
    slots, _, height, width = got.shape
    to = [lax.rem(g + d, groups) for d in dist]

    barrier = pltpu.get_barrier_semaphore()
    steps = sorted({d for d in dist} | {(groups - d) % groups for d in dist} | {0})
    for e in steps:
        for m in range(rows):
            if e == 0 and m == 0:
                continue
            pl.semaphore_signal(barrier, inc=1, device_id={"row": r ^ m, "expert": lax.rem(g + e, groups)},
                                device_id_type=MESH)
    pl.semaphore_wait(barrier, len(steps) * rows - 1)

    def remote(src, dst, s, t, row, expert):
        return pltpu.make_async_remote_copy(src_ref=src, dst_ref=dst, send_sem=s, recv_sem=t,
                                            device_id={"row": row, "expert": expert}, device_id_type=MESH)

    first = []
    for j in range(slots):
        for src, dst, s, t in (
            (left.at[j], left_all.at[j, r], lsend.at[j, 0], lrecv.at[j, 0]),
            (right.at[j], right_got.at[j], ssend.at[j, 0], srecv.at[j, 0]),
            (scale.at[j], scale_got.at[j], ssend.at[j, 1], srecv.at[j, 1]),
        ):
            if dist[j] == 0:
                copy = pltpu.make_async_copy(src, dst, t)
            else:
                copy = remote(src, dst, s, t, r, to[j])
            copy.start()
            first.append(copy)

    def left_round(mask, held):
        copies = []
        for s in held:
            for j in range(slots):
                piece = left_all.at[j, r ^ s]
                copy = remote(piece, piece, lsend.at[j, mask | s], lrecv.at[j, mask | s], r ^ mask, g)
                copy.start()
                copies.append(copy)
        return copies

    rounds = []
    mask, held = rows // 2, [0]
    while mask:
        rounds.append((mask, list(held)))
        held += [s | mask for s in held]
        mask //= 2

    pieces = [(m, j) for m in piece_order(rows) for j in range(slots)]
    at = {1 + i * (len(pieces) // len(rounds)): i for i in range(len(rounds))}
    pending, waiting = [], first
    for k, (m, j) in enumerate(pieces):
        if k in at:
            for copy in waiting:
                copy.wait()
            waiting = left_round(*rounds[at[k]])
        if len(pending) >= WINDOW:
            pending.pop(0).wait_send()
        c = r ^ m
        src = base.at[j, :, pl.ds(pl.multiple_of(c * width, width), width)]
        if m == 0 and dist[j] == 0:
            pltpu.make_async_copy(src, got.at[j, r], recv.at[j, 0]).start()
        else:
            copy = remote(src, got.at[j, r], send.at[j, m], recv.at[j, m], c, to[j])
            copy.start()
            pending.append(copy)
    for copy in waiting:
        copy.wait()

    unit = next(u for u in (1, 2, 4, 8) if u * height % LANES == 0)
    half = rows // 2
    turns = rows * slots // unit

    def place(t):
        q, f, j = t // (2 * slots) * unit, t // slots % 2, t % slots
        m = (1 - f) * (half + q) + f * ((half // 2 + q) % half)
        return m, j, (r ^ m) // unit * unit

    def written(t):
        m, j, row = place(t)
        rows_of = pl.ds(pl.multiple_of(row, unit), unit)
        return pltpu.make_async_copy(got.at[j, rows_of], out.at[j, rows_of], osem.at[t])

    def turn(t, carry):
        m, j, row = place(t)
        for u in range(unit):
            block = got.at[j, r ^ (m + u)]
            remote(block, block, send.at[j, m + u], recv.at[j, m + u], r ^ 1, g).wait_recv()
        rank_all = left_all.shape[1] * left_all.shape[2]
        columns = pl.ds(pl.multiple_of(row * height, LANES), unit * height)
        a = left_all[j, :, :, columns].reshape(rank_all, unit * height)
        delta = lax.dot_general(a, right_got[j], (((0,), (0,)), ((), ())), preferred_element_type=jnp.float32)
        weight = scale_got[j, 0:1, 0:1]
        for u in range(unit):
            part = delta[u * height:(u + 1) * height]
            got[j, row + u] = (got[j, row + u].astype(jnp.float32) + weight * part).astype(got.dtype)
        written(t).start()
        return carry

    lax.fori_loop(0, turns, turn, 0)
    for copy in pending:
        copy.wait_send()

    def settle(t, carry):
        written(t).wait()
        return carry

    lax.fori_loop(0, turns, settle, 0)


def exchange(first, groups, rows, base, left, right, scale):
    dist = (first, groups - 1 - first)
    slots, height, total = base.shape
    width = total // rows
    rank, model = left.shape[1:]
    anywhere = pl.BlockSpec(memory_space=pl.ANY)
    dma = pltpu.SemaphoreType.DMA
    return pl.pallas_call(
        functools.partial(exchange_kernel, dist, groups, rows),
        out_shape=jax.ShapeDtypeStruct((slots, rows, height, width), base.dtype),
        in_specs=[anywhere] * 4,
        out_specs=anywhere,
        scratch_shapes=[
            pltpu.VMEM((slots, rows, height, width), base.dtype),
            pltpu.VMEM((slots, rows, rank, model), left.dtype),
            pltpu.VMEM(right.shape, right.dtype),
            pltpu.VMEM(scale.shape, scale.dtype),
            dma((slots, rows)), dma((slots, rows)),
            dma((slots, rows)), dma((slots, rows)),
            dma((slots, 2)), dma((slots, 2)),
            dma((slots * rows,)),
        ],
        compiler_params=pltpu.CompilerParams(collective_id=first, has_side_effects=True),
        name=f"exchange_{first}",
    )(base, left, right, scale)


def local(groups, rows, base, left_factors, right_factors, expert_adapter_scale, placement):
    first = jnp.mod(placement[0] - lax.axis_index("expert"), groups)
    slots = base.shape[0]
    left = jnp.swapaxes(left_factors, 1, 2)
    scale = jnp.broadcast_to(expert_adapter_scale[:, None, None], (slots, 8, 128))
    served = lax.switch(
        first,
        [functools.partial(exchange, o, groups, rows) for o in range(groups)],
        base, left, right_factors, scale,
    )
    return served.reshape(slots, left.shape[2], served.shape[3])


def solution(mesh):
    placed = (
        P("expert", "row", None),
        P("expert", None, "row"),
        P("expert", None, "row"),
        P("expert"),
        P("expert"),
    )
    return jax.shard_map(
        functools.partial(local, mesh.shape["expert"], mesh.shape["row"]),
        mesh=mesh, in_specs=placed, out_specs=P("expert", None, "row"), check_vma=False,
    )
```

```python
import functools

import jax
import jax.numpy as jnp
from jax import lax
from jax.experimental import pallas as pl
from jax.experimental.pallas import tpu as pltpu
from jax.sharding import PartitionSpec as P

MESH = pl.DeviceIdType.MESH
WINDOW = 8
LANES = 128


def unit_of(height):
    return next(u for u in (1, 2, 4, 8) if u * height % LANES == 0)


def near_turn(q, half):
    quarter = half // 2
    return (q + q // quarter) % half + quarter * (1 - (q + half - 1) // half)


def piece_order(rows, unit):
    half = rows // 2
    order = []
    for q in range(half // unit):
        for m in (half + q * unit, near_turn(q, half // unit) * unit):
            order += range(m, m + unit)
    return order


def exchange_kernel(dist, groups, rows, base, left, right, scale, out, got, left_all, right_got, scale_got,
                    send, recv, lsend, lrecv, ssend, srecv, osem):
    r, g = lax.axis_index("row"), lax.axis_index("expert")
    slots, _, height, width = got.shape
    to = [lax.rem(g + d, groups) for d in dist]

    barrier = pltpu.get_barrier_semaphore()
    steps = sorted({d for d in dist} | {(groups - d) % groups for d in dist} | {0})
    for e in steps:
        for m in range(rows):
            if e == 0 and m == 0:
                continue
            pl.semaphore_signal(barrier, inc=1, device_id={"row": r ^ m, "expert": lax.rem(g + e, groups)},
                                device_id_type=MESH)
    pl.semaphore_wait(barrier, len(steps) * rows - 1)

    def remote(src, dst, s, t, row, expert):
        return pltpu.make_async_remote_copy(src_ref=src, dst_ref=dst, send_sem=s, recv_sem=t,
                                            device_id={"row": row, "expert": expert}, device_id_type=MESH)

    first = []
    for j in range(slots):
        for src, dst, s, t in (
            (left.at[j], left_all.at[j, r], lsend.at[j, 0], lrecv.at[j, 0]),
            (right.at[j], right_got.at[j], ssend.at[j, 0], srecv.at[j, 0]),
            (scale.at[j], scale_got.at[j], ssend.at[j, 1], srecv.at[j, 1]),
        ):
            if dist[j] == 0:
                copy = pltpu.make_async_copy(src, dst, t)
            else:
                copy = remote(src, dst, s, t, r, to[j])
            copy.start()
            first.append(copy)

    def left_round(mask, held):
        copies = []
        for s in held:
            for j in range(slots):
                piece = left_all.at[j, r ^ s]
                copy = remote(piece, piece, lsend.at[j, mask | s], lrecv.at[j, mask | s], r ^ mask, g)
                copy.start()
                copies.append(copy)
        return copies

    rounds = []
    mask, held = rows // 2, [0]
    while mask:
        rounds.append((mask, list(held)))
        held += [s | mask for s in held]
        mask //= 2

    pieces = [(m, j) for m in piece_order(rows, unit_of(height)) for j in range(slots)]
    at = {1 + i * (len(pieces) // len(rounds)): i for i in range(len(rounds))}
    pending, waiting = [], first
    for k, (m, j) in enumerate(pieces):
        if k in at:
            for copy in waiting:
                copy.wait()
            waiting = left_round(*rounds[at[k]])
        if len(pending) >= WINDOW:
            pending.pop(0).wait_send()
        c = r ^ m
        src = base.at[j, :, pl.ds(pl.multiple_of(c * width, width), width)]
        if m == 0 and dist[j] == 0:
            pltpu.make_async_copy(src, got.at[j, r], recv.at[j, 0]).start()
        else:
            copy = remote(src, got.at[j, r], send.at[j, m], recv.at[j, m], c, to[j])
            copy.start()
            pending.append(copy)
    for copy in waiting:
        copy.wait()

    unit = unit_of(height)
    half = rows // 2
    turns = rows * slots // unit

    def place(t):
        q, f, j = t // (2 * slots), t // slots % 2, t % slots
        m = (1 - f) * (half + q * unit) + f * near_turn(q, half // unit) * unit
        return m, j, (r ^ m) // unit * unit

    def written(t):
        m, j, row = place(t)
        rows_of = pl.ds(pl.multiple_of(row, unit), unit)
        return pltpu.make_async_copy(got.at[j, rows_of], out.at[j, rows_of], osem.at[t])

    def turn(t, carry):
        m, j, row = place(t)
        for u in range(unit):
            block = got.at[j, r ^ (m + u)]
            remote(block, block, send.at[j, m + u], recv.at[j, m + u], r ^ 1, g).wait_recv()
        rank_all = left_all.shape[1] * left_all.shape[2]
        columns = pl.ds(pl.multiple_of(row * height, LANES), unit * height)
        a = left_all[j, :, :, columns].reshape(rank_all, unit * height)
        delta = lax.dot_general(a, right_got[j], (((0,), (0,)), ((), ())), preferred_element_type=jnp.float32)
        weight = scale_got[j, 0:1, 0:1]
        for u in range(unit):
            part = delta[u * height:(u + 1) * height]
            got[j, row + u] = (got[j, row + u].astype(jnp.float32) + weight * part).astype(got.dtype)
        written(t).start()
        return carry

    lax.fori_loop(0, turns, turn, 0)
    for copy in pending:
        copy.wait_send()

    def settle(t, carry):
        written(t).wait()
        return carry

    lax.fori_loop(0, turns, settle, 0)


def exchange(first, groups, rows, base, left, right, scale):
    dist = (first, groups - 1 - first)
    slots, height, total = base.shape
    width = total // rows
    rank, model = left.shape[1:]
    anywhere = pl.BlockSpec(memory_space=pl.ANY)
    dma = pltpu.SemaphoreType.DMA
    return pl.pallas_call(
        functools.partial(exchange_kernel, dist, groups, rows),
        out_shape=jax.ShapeDtypeStruct((slots, rows, height, width), base.dtype),
        in_specs=[anywhere] * 4,
        out_specs=anywhere,
        scratch_shapes=[
            pltpu.VMEM((slots, rows, height, width), base.dtype),
            pltpu.VMEM((slots, rows, rank, model), left.dtype),
            pltpu.VMEM(right.shape, right.dtype),
            pltpu.VMEM(scale.shape, scale.dtype),
            dma((slots, rows)), dma((slots, rows)),
            dma((slots, rows)), dma((slots, rows)),
            dma((slots, 2)), dma((slots, 2)),
            dma((slots * rows,)),
        ],
        compiler_params=pltpu.CompilerParams(collective_id=first, has_side_effects=True),
        name=f"exchange_{first}",
    )(base, left, right, scale)


def local(groups, rows, base, left_factors, right_factors, expert_adapter_scale, placement):
    first = jnp.mod(placement[0] - lax.axis_index("expert"), groups)
    slots = base.shape[0]
    left = jnp.swapaxes(left_factors, 1, 2)
    scale = jnp.broadcast_to(expert_adapter_scale[:, None, None], (slots, 8, 128))
    served = lax.switch(
        first,
        [functools.partial(exchange, o, groups, rows) for o in range(groups)],
        base, left, right_factors, scale,
    )
    return served.reshape(slots, left.shape[2], served.shape[3])


def solution(mesh):
    placed = (
        P("expert", "row", None),
        P("expert", None, "row"),
        P("expert", None, "row"),
        P("expert"),
        P("expert"),
    )
    return jax.shard_map(
        functools.partial(local, mesh.shape["expert"], mesh.shape["row"]),
        mesh=mesh, in_specs=placed, out_specs=P("expert", None, "row"), check_vma=False,
    )
```

```python
import functools

import jax
import jax.numpy as jnp
from jax import lax
from jax.experimental import pallas as pl
from jax.experimental.pallas import tpu as pltpu
from jax.sharding import PartitionSpec as P

MESH = pl.DeviceIdType.MESH
WINDOW = 8
LANES = 128


def unit_of(height):
    return next(u for u in (1, 2, 4, 8) if u * height % LANES == 0)


def near_turn(q, half):
    quarter = half // 2
    return (q + q // quarter) % half + quarter * (1 - (q + half - 1) // half)


def piece_order(rows, unit):
    half = rows // 2
    order = []
    for q in range(half // unit):
        for m in (half + q * unit, near_turn(q, half // unit) * unit):
            order += range(m, m + unit)
    return order


def exchange_kernel(dist, groups, rows, base, left, right, scale, out, got, left_all, right_got, scale_got,
                    send, recv, lsend, lrecv, ssend, srecv, osem):
    r, g = lax.axis_index("row"), lax.axis_index("expert")
    slots, _, height, width = got.shape
    to = [lax.rem(g + d, groups) for d in dist]

    barrier = pltpu.get_barrier_semaphore()
    steps = sorted({d for d in dist} | {(groups - d) % groups for d in dist} | {0})
    for e in steps:
        for m in range(rows):
            if e == 0 and m == 0:
                continue
            pl.semaphore_signal(barrier, inc=1, device_id={"row": r ^ m, "expert": lax.rem(g + e, groups)},
                                device_id_type=MESH)
    pl.semaphore_wait(barrier, len(steps) * rows - 1)

    def remote(src, dst, s, t, row, expert):
        return pltpu.make_async_remote_copy(src_ref=src, dst_ref=dst, send_sem=s, recv_sem=t,
                                            device_id={"row": row, "expert": expert}, device_id_type=MESH)

    first = []
    for j in range(slots):
        for src, dst, s, t in (
            (left.at[j], left_all.at[j, r], lsend.at[j, 0], lrecv.at[j, 0]),
            (right.at[j], right_got.at[j], ssend.at[j, 0], srecv.at[j, 0]),
            (scale.at[j], scale_got.at[j], ssend.at[j, 1], srecv.at[j, 1]),
        ):
            if dist[j] == 0:
                copy = pltpu.make_async_copy(src, dst, t)
            else:
                copy = remote(src, dst, s, t, r, to[j])
            copy.start()
            first.append(copy)

    def left_round(mask, held):
        copies = []
        for s in held:
            for j in range(slots):
                piece = left_all.at[j, r ^ s]
                copy = remote(piece, piece, lsend.at[j, mask | s], lrecv.at[j, mask | s], r ^ mask, g)
                copy.start()
                copies.append(copy)
        return copies

    rounds = []
    mask, held = rows // 2, [0]
    while mask:
        rounds.append((mask, list(held)))
        held += [s | mask for s in held]
        mask //= 2

    pieces = [(m, j) for m in piece_order(rows, unit_of(height)) for j in range(slots)]
    at = {1 + i * (len(pieces) // len(rounds)): i for i in range(len(rounds))}
    pending, waiting = [], first
    for k, (m, j) in enumerate(pieces):
        if k in at:
            for copy in waiting:
                copy.wait()
            waiting = left_round(*rounds[at[k]])
        if len(pending) >= WINDOW:
            pending.pop(0).wait_send()
        c = r ^ m
        src = base.at[j, :, pl.ds(pl.multiple_of(c * width, width), width)]
        if m == 0 and dist[j] == 0:
            pltpu.make_async_copy(src, got.at[j, r], recv.at[j, 0]).start()
        else:
            copy = remote(src, got.at[j, r], send.at[j, m], recv.at[j, m], c, to[j])
            copy.start()
            pending.append(copy)
    for copy in waiting:
        copy.wait()

    unit = unit_of(height)
    half = rows // 2
    turns = rows * slots // unit

    def place(t):
        q, f, j = t // (2 * slots), t // slots % 2, t % slots
        m = (1 - f) * (half + q * unit) + f * near_turn(q, half // unit) * unit
        return m, j, (r ^ m) // unit * unit

    def written(t):
        m, j, row = place(t)
        rows_of = pl.ds(pl.multiple_of(row, unit), unit)
        return pltpu.make_async_copy(got.at[j, rows_of], out.at[j, rows_of], osem.at[t])

    def turn(t, carry):
        m, j, row = place(t)
        for u in range(unit):
            block = got.at[j, r ^ (m + u)]
            remote(block, block, send.at[j, m + u], recv.at[j, m + u], r ^ 1, g).wait_recv()
        rank_all = left_all.shape[1] * left_all.shape[2]
        columns = pl.ds(pl.multiple_of(row * height, LANES), unit * height)
        a = left_all[j, :, :, columns].reshape(rank_all, unit * height)
        delta = lax.dot_general(a, right_got[j], (((0,), (0,)), ((), ())), preferred_element_type=jnp.float32)
        weight = scale_got[j, 0:1, 0:1]
        for u in range(unit):
            part = delta[u * height:(u + 1) * height]
            got[j, row + u] = (got[j, row + u].astype(jnp.float32) + weight * part).astype(got.dtype)
        written(t).start()
        return carry

    lax.fori_loop(0, turns, turn, 0)
    for copy in pending:
        copy.wait_send()

    def settle(t, carry):
        written(t).wait()
        return carry

    lax.fori_loop(0, turns, settle, 0)


def exchange(first, groups, rows, base, left, right, scale):
    dist = (first, groups - 1 - first)
    slots, height, total = base.shape
    width = total // rows
    rank, model = left.shape[1:]
    anywhere = pl.BlockSpec(memory_space=pl.ANY)
    dma = pltpu.SemaphoreType.DMA
    return pl.pallas_call(
        functools.partial(exchange_kernel, dist, groups, rows),
        out_shape=jax.ShapeDtypeStruct((slots, rows, height, width), base.dtype),
        in_specs=[anywhere] * 4,
        out_specs=anywhere,
        scratch_shapes=[
            pltpu.VMEM((slots, rows, height, width), base.dtype),
            pltpu.VMEM((slots, rows, rank, model), left.dtype),
            pltpu.VMEM(right.shape, right.dtype),
            pltpu.VMEM(scale.shape, scale.dtype),
            dma((slots, rows)), dma((slots, rows)),
            dma((slots, rows)), dma((slots, rows)),
            dma((slots, 2)), dma((slots, 2)),
            dma((slots * rows,)),
        ],
        compiler_params=pltpu.CompilerParams(collective_id=first, has_side_effects=True),
        name=f"exchange_{first}",
    )(base, left, right, scale)


def copy_out_kernel(chunks, x, y, held, rsem, wsem):
    size = x.shape[1] // chunks
    reads, writes = [], []
    for j in range(x.shape[0]):
        for i in range(chunks):
            here = pl.ds(i * size, size)
            reads.append(pltpu.make_async_copy(x.at[j, here], held.at[j, here], rsem.at[j, i]))
            writes.append(pltpu.make_async_copy(held.at[j, here], y.at[j, here], wsem.at[j, i]))
    for copy in reads:
        copy.start()
    for read, write in zip(reads, writes):
        read.wait()
        write.start()
    for copy in writes:
        copy.wait()


def copy_out(x, chunks=7):
    dma = pltpu.SemaphoreType.DMA
    anywhere = pl.BlockSpec(memory_space=pl.ANY)
    return pl.pallas_call(
        functools.partial(copy_out_kernel, chunks),
        out_shape=jax.ShapeDtypeStruct(x.shape, x.dtype),
        in_specs=[anywhere],
        out_specs=anywhere,
        scratch_shapes=[pltpu.VMEM(x.shape, x.dtype), dma((x.shape[0], chunks)), dma((x.shape[0], chunks))],
        name="copy_out",
    )(x)


def local(groups, rows, base, left_factors, right_factors, expert_adapter_scale, placement):
    first = jnp.mod(placement[0] - lax.axis_index("expert"), groups)
    slots = base.shape[0]
    left = jnp.swapaxes(left_factors, 1, 2)
    scale = jnp.broadcast_to(expert_adapter_scale[:, None, None], (slots, 8, 128))
    served = lax.switch(
        first,
        [functools.partial(exchange, o, groups, rows) for o in range(groups)],
        base, left, right_factors, scale,
    )
    return copy_out(served.reshape(slots, left.shape[2], served.shape[3]))


def solution(mesh):
    placed = (
        P("expert", "row", None),
        P("expert", None, "row"),
        P("expert", None, "row"),
        P("expert"),
        P("expert"),
    )
    return jax.shard_map(
        functools.partial(local, mesh.shape["expert"], mesh.shape["row"]),
        mesh=mesh, in_specs=placed, out_specs=P("expert", None, "row"), check_vma=False,
    )
```
